128 devices in a mesh: node: 128 (over z, x, y, core).
Axes of the slice: x: 4, y: 4, z: 4, core: 2. Of those that a mesh axis runs over, the one named last changes fastest.
Arguments:
- labels: bfloat16 [524288, 512], P('node'), may hold values from -6 to 6
- seed_mask: int32 [524288], P('node'), may hold values 0 or 1
- band_w: bfloat16 [4096, 3, 128, 128], P('node'), may hold values from 0.0009994507 to 1
- far_block: int32 [128, 128, 2], P('node'), may hold values from 0 to 511
- far_tile: int32 [128, 128, 2], P('node'), may hold values from 0 to 31
- far_count: int32 [128, 128], P('node'), may hold values from 0 to 2, as said below
- far_w: bfloat16 [128, 128, 2, 8, 128], P('node'), may hold values from 0.049804688 to 2
Outputs:
- final_labels: bfloat16 [524288, 512], P('node')
- residual: float32 [2, 4096], P(None, 'node')
The draws below stay inside these ranges and needn't reach their ends.
Inputs may be any that keep to these rules, and one draw needn't show every extreme that they name: `far_count`: in every draw at least one destination shard has all 2 slots live from every source shard; other counts vary from pair to pair.
All inputs are finite; a program needn't handle non-finite values. No bound on the sum of `seed_mask` on one device may be relied on, other than what follows from the above.
Results may differ from the reference program's by a relative error of at most 0.0027.
Values may be sent and summed in bfloat16 or wider, within the bound.
No kernel may reach another device: no remote copies, remote signals or barrier semaphores. Data moves between devices by JAX's collectives and lax.ppermute only.
A program may use at most 128 MiB of HBM per device.

```python
import math
import jax
import jax.numpy as jnp
from jax import lax

C = 512
NODE_DEV = 4096
TILE = 128
BLK = 8
SLOTS = 2
ITERS = 2
NODES = 524288
N_NODE = 128


def draw_far_count(key, part):
    first_key, second_key = jax.random.split(jax.random.fold_in(key, 17))
    counts = jax.random.randint(first_key, (N_NODE, N_NODE), 0, SLOTS + 1)
    busiest = jax.random.randint(second_key, (), 0, N_NODE)
    row_ids = jnp.arange(N_NODE)[:, None]
    return jnp.where(row_ids == busiest, SLOTS, counts).astype(jnp.int32)


def set_ends(values, rng, smallest, top_value):
    dims = values.shape
    place = [jax.random.randint(jax.random.fold_in(rng, axis), (), 0, dims[axis]) for axis in range(len(dims))]
    values = values.at[tuple(place)].set(smallest)
    longest = dims.index(max(dims))
    place[longest] = (place[longest] + 1) % dims[longest]
    return values.at[tuple(place)].set(top_value)


def block_scale(own_key, dims, cuts, smallest, high):
    factor_of, own = 1.0, jax.random.fold_in(own_key, 6)
    for dim, parts in cuts:
        steps = jnp.exp(jax.random.uniform(jax.random.fold_in(own, dim), (parts,), jnp.float32, smallest / len(cuts), high / len(cuts)))
        factor_of = factor_of * jnp.repeat(steps, dims[dim] // parts).reshape([-1 if axis == dim else 1 for axis in range(len(dims))])
    return factor_of


def normal_values(own_key, shape, width, most, pieces=(), dtype=jnp.bfloat16):
    array = width * jax.random.normal(own_key, shape, jnp.float32)
    if pieces:
        array = array * block_scale(own_key, shape, pieces, -0.22, 0.18)
    return jnp.clip(array, -most, most).astype(dtype)


def setup_inputs(seed: int = 0) -> dict:
    key_of = jax.random.split(jax.random.key(seed), 8)
    return {
        "labels": normal_values(key_of[0], (NODES, C), 1.0, 6.0, ((0, 128),)),
        "seed_mask": set_ends((jax.random.randint(key_of[1], (NODES,), 0, 4) < 1).astype(jnp.int32), jax.random.fold_in(key_of[1], 1), 0, 1),
        "band_w": jnp.clip(jnp.exp(math.log(1.0) - 6.9083047 * jax.random.uniform(key_of[2], (NODES // TILE, 3, TILE, TILE), jnp.float32) ** block_scale(key_of[2], (NODES // TILE, 3, TILE, TILE), ((0, 128),), -0.2, 0.2)), 0.0009994507, 1.0).astype(jnp.bfloat16),
        "far_block": set_ends(jax.random.randint(key_of[3], (N_NODE, N_NODE, SLOTS), 0, NODE_DEV // BLK), jax.random.fold_in(key_of[3], 1), 0, (NODE_DEV // BLK) - 1).astype(jnp.int32),
        "far_tile": set_ends(jax.random.randint(key_of[4], (N_NODE, N_NODE, SLOTS), 0, NODE_DEV // TILE), jax.random.fold_in(key_of[4], 1), 0, (NODE_DEV // TILE) - 1).astype(jnp.int32),
        "far_count": draw_far_count(jax.random.fold_in(key_of[7], 71), 0),
        "far_w": jnp.clip(jnp.exp(math.log(2.0) - 3.6927934 * jax.random.uniform(key_of[6], (N_NODE, N_NODE, SLOTS, BLK, TILE), jnp.float32) ** block_scale(key_of[6], (N_NODE, N_NODE, SLOTS, BLK, TILE), ((0, 128),), -0.2, 0.2)), 0.049804688, 2.0).astype(jnp.bfloat16),
    }


def live_table(count_row):
    return (jnp.arange(SLOTS)[None, :] < count_row[:, None]).astype(jnp.float32)

def reference(labels, seed_mask, band_w, far_block, far_tile, far_count, far_w):
    tile_total = labels.shape[0] // TILE
    block_count = NODE_DEV // BLK
    band_wide = band_w.astype(jnp.float32)
    degree_band = lax.optimization_barrier(jnp.sum(band_wide, axis=(1, 3)))

    def far_degree(packed):
        tiles_here, count_here, weight_here = packed
        live_weights = weight_here.astype(jnp.float32) * live_table(count_here)[:, :, None, None]
        weight_sums = lax.optimization_barrier(jnp.sum(live_weights, axis=2)).reshape(-1, TILE)
        return jnp.zeros((NODE_DEV // TILE, TILE), jnp.float32).at[tiles_here.reshape(-1)].add(weight_sums)
    degree_far = lax.map(far_degree, (far_tile, far_count, far_w)).reshape(tile_total, TILE)
    degree = degree_band + degree_far
    seeded = (seed_mask == 1).reshape(tile_total, TILE, 1)
    clamped = labels.astype(jnp.float32).reshape(tile_total, TILE, C)
    current = labels
    residuals = []
    for sweep in range(ITERS):
        tiles = current.astype(jnp.float32).reshape(tile_total, TILE, C)
        band_sum = jnp.zeros((tile_total, TILE, C), jnp.float32)
        for offset in (-1, 0, 1):
            source = jnp.roll(tiles, -offset, axis=0)
            band_sum = band_sum + jnp.einsum('itr,irc->itc', band_wide[:, offset + 1], source)
        blocks_all = current.reshape(N_NODE, block_count, BLK, C)

        def far_part(packed):
            wanted, tiles_here, count_here, weight_here = packed
            blocks = blocks_all[jnp.arange(N_NODE)[:, None], wanted].astype(jnp.float32)
            live_weights = weight_here.astype(jnp.float32) * live_table(count_here)[:, :, None, None]
            contrib = jnp.einsum('skqt,skqc->sktc', live_weights, blocks)
            return jnp.zeros((NODE_DEV // TILE, TILE, C), jnp.float32).at[tiles_here.reshape(-1)].add(contrib.reshape(-1, TILE, C))
        far_sum = lax.map(far_part, (far_block, far_tile, far_count, far_w)).reshape(tile_total, TILE, C)
        averaged = (band_sum + far_sum) / degree[:, :, None]
        row_scale = jnp.sqrt(lax.optimization_barrier(jnp.mean(averaged * averaged, axis=2, keepdims=True)))
        scaled = averaged / jnp.maximum(row_scale, 0.05)
        fresh = jnp.where(seeded, clamped, scaled).astype(jnp.bfloat16)
        residuals.append(lax.optimization_barrier(jnp.sum(jnp.abs(fresh.astype(jnp.float32) - tiles), axis=(1, 2))))
        current = fresh.reshape(labels.shape[0], C)
    return (current, jnp.stack(residuals))
```

```python
import jax
import jax.numpy as jnp
from jax import lax
from jax.experimental import pallas as pl
from jax.experimental.pallas import tpu as pltpu
from jax.sharding import PartitionSpec as P

ITERS = 2
CAP = 16
GROUP = 4
F32 = jnp.float32
BF16 = jnp.bfloat16
VMEM = pl.BlockSpec(memory_space=pltpu.VMEM)
SMEM = pl.BlockSpec(memory_space=pltpu.SMEM)
ANY = pl.BlockSpec(memory_space=pltpu.HBM)
MIB = 1 << 20
DMA = pltpu.SemaphoreType.DMA


def in_hbm(x):
    return pltpu.with_memory_space_constraint(x, pltpu.HBM)


def in_vmem(x):
    return pltpu.with_memory_space_constraint(x, pltpu.VMEM)


def dot(a, b):
    return jnp.dot(a, b, preferred_element_type=F32)


def loop(low, high, step, unroll=1):
    def run(i, carry):
        step(i)
        return carry

    lax.fori_loop(low, high, run, 0, unroll=unroll)


def fold(row, width):
    total = row[:, :width]
    for j in range(1, row.shape[1] // width):
        total = total + row[:, j * width : (j + 1) * width]
    return total


def pick_kernel(got_ref, cur_ref, req_ref, send_ref, flat_ref, word_ref, held_ref, word_sem, in_sem, out_sem):
    slots, peers = req_ref.shape
    table = jnp.concatenate([got_ref[:, 0, :], jnp.zeros((peers, peers - slots), jnp.int32)], axis=1)
    flat_ref[...] = table.T[:8, :]
    move = pltpu.make_async_copy(flat_ref.at[pl.ds(0, slots)], word_ref, word_sem)
    move.start()
    move.wait()
    parts = in_sem.shape[0]
    share = peers // parts

    def fetch(d, part):
        for k in range(slots):
            row = word_ref[k, d]
            req_ref[k, d] = row
            pltpu.make_async_copy(cur_ref.at[row], held_ref.at[d * slots + k], in_sem.at[part]).start()

    for part in range(parts):
        loop(part * share, (part + 1) * share, lambda d: fetch(d, part), unroll=4)
    for part in range(parts):
        here = pl.ds(part * share * slots, share * slots)
        pltpu.make_async_copy(held_ref.at[here], held_ref.at[here], in_sem.at[part]).wait()
        pltpu.make_async_copy(held_ref.at[here], send_ref.at[here], out_sem.at[part]).start()
    for part in range(parts):
        here = pl.ds(part * share * slots, share * slots)
        pltpu.make_async_copy(held_ref.at[here], send_ref.at[here], out_sem.at[part]).wait()


def pick_blocks(got, blocks):
    peers, _, slots = got.shape
    shape = (peers * slots,) + blocks.shape[1:]
    return pl.pallas_call(
        pick_kernel,
        out_shape=(jax.ShapeDtypeStruct((slots, peers), jnp.int32), pltpu.HBM(shape, BF16)),
        in_specs=[VMEM, ANY],
        out_specs=(SMEM, ANY),
        scratch_shapes=[
            pltpu.VMEM((8, peers), jnp.int32),
            pltpu.SMEM((slots, peers), jnp.int32),
            pltpu.VMEM(shape, BF16),
            DMA,
            DMA((4,)),
            DMA((4,)),
        ],
        cost_estimate=pl.CostEstimate(flops=1_000_000_000, bytes_accessed=4_000_000, transcendentals=0),
        compiler_params=pltpu.CompilerParams(vmem_limit_bytes=32 * MIB),
        name="pick",
    )(in_vmem(got), in_hbm(blocks))


def band_sum(band_ref, cur_ref, t, tiles, rows):
    def rows_of(first, n):
        return cur_ref[pl.ds(pl.multiple_of(first * rows, rows), n * rows), :]

    def join(offsets):
        return jnp.concatenate([band_ref[t, o] for o in offsets], axis=1)

    if isinstance(t, int) and t == 0:
        return dot(join((1, 2)), rows_of(0, 2))
    if isinstance(t, int) and t == tiles - 1:
        return dot(join((0, 1)), rows_of(tiles - 2, 2))
    return dot(join((0, 1, 2)), rows_of(t - 1, 3))


def prep_kernel(
    tile_ref, count_ref, seed_ref, far_ref, band_hbm, lab_hbm,
    table_ref, mat_hbm, aux_ref, edge_ref, base_hbm,
    cnt_ref, num_ref, band_ref, lab_ref, out_ref, deg_ref, mat_ref, in_sem, out_sem, mat_sem,
):
    peers = count_ref.shape[0]
    total = tile_ref.shape[0]
    slots = total // peers
    tiles, _, rows, _ = band_ref.shape
    chunks = mat_ref.shape[0]
    num_at, ext_at, used_at = chunks * CAP, chunks * CAP + tiles, chunks * CAP + chunks
    get_band = pltpu.make_async_copy(band_hbm, band_ref, in_sem.at[0])
    get_lab = pltpu.make_async_copy(lab_hbm, lab_ref, in_sem.at[1])
    get_band.start()
    get_lab.start()

    def clear(i):
        table_ref[i] = 0

    loop(0, table_ref.shape[0], clear, unroll=16)

    def clear_count(i):
        cnt_ref[i] = 0
        num_ref[i] = 0

    loop(0, chunks, clear_count, unroll=8)

    def scan(peer):
        live = count_ref[peer]
        for k in range(slots):
            @pl.when(k < live)
            def _():
                tile = tile_ref[k * peers + peer]
                place = num_ref[tile]
                num_ref[tile] = place + 1
                slot = peer * slots + k

                @pl.when(place < CAP)
                def _():
                    table_ref[tile * CAP + place] = slot

                @pl.when(place >= CAP)
                def _():
                    inner = lax.rem(place, CAP)

                    @pl.when(inner == 0)
                    def _():
                        fresh = table_ref[used_at]
                        table_ref[ext_at + fresh] = tile
                        table_ref[used_at] = fresh + 1

                    def find(c, last):
                        return jnp.where(table_ref[ext_at + c] == tile, c, last)

                    chunk = tiles + lax.fori_loop(0, table_ref[used_at], find, 0)
                    table_ref[chunk * CAP + inner] = slot
                    cnt_ref[chunk] = inner + 1

    loop(0, peers, scan, unroll=2)

    def tidy(t):
        cnt_ref[t] = jnp.minimum(num_ref[t], CAP)
        table_ref[num_at + t] = num_ref[t]

    loop(0, tiles, tidy)

    def seeded(t):
        return jnp.broadcast_to(seed_ref[t].astype(F32), (rows, rows)).T == 1.0

    def build(c, free):
        parts = [far_ref[table_ref[c * CAP + p]].astype(F32) for p in range(CAP)]
        mat = jnp.concatenate(parts, axis=0)
        depth = lax.broadcasted_iota(jnp.int32, mat.shape, 0)
        mat = jnp.where(depth < cnt_ref[c] * far_ref.shape[1], mat, 0.0).T
        mat_ref[c] = jnp.where(free, mat, 0.0).astype(BF16)
        return mat

    get_band.wait()
    get_lab.wait()

    def copy_of(t):
        return pltpu.make_async_copy(out_ref.at[t], base_hbm.at[t], out_sem.at[t])

    def tile_step(t):
        seed = seeded(t)
        free = jnp.logical_not(seed)
        w = band_ref[t].astype(F32)
        degree = jnp.sum(w[0] + w[1] + w[2] + build(t, free), axis=1, keepdims=True)
        deg_ref[t] = jnp.broadcast_to(degree, (rows, rows))
        here = lab_ref[pl.ds(pl.multiple_of(t * rows, rows), rows), :].astype(F32)
        out_ref[t] = jnp.where(seed[:, :1], here, band_sum(band_ref, lab_ref, t, tiles, rows))
        copy_of(t).start()

    tile_step(0)
    loop(1, tiles - 1, tile_step)
    tile_step(tiles - 1)

    def extra_step(c):
        t = table_ref[ext_at + c]
        mat = build(tiles + c, jnp.logical_not(seeded(t)))
        deg_ref[t] = deg_ref[t] + jnp.sum(mat, axis=1, keepdims=True)

    loop(0, table_ref[used_at], extra_step)
    put_mat = pltpu.make_async_copy(mat_ref, mat_hbm, mat_sem)
    put_mat.start()
    lane = lax.broadcasted_iota(jnp.int32, (rows, rows), 1)
    aux_ref[...] = jnp.ones_like(aux_ref)

    def finish(t):
        inv = 1.0 / deg_ref[t]
        aux_ref[...] = jnp.where(lane == t, jnp.where(seeded(t), -inv, inv), aux_ref[...])

    loop(0, tiles, finish)
    for side, (t, o) in enumerate(((0, 0), (tiles - 1, 2))):
        edge_ref[side] = jnp.where(seeded(t), 0.0, band_ref[t, o].astype(F32)).astype(BF16)
    loop(0, tiles, lambda t: copy_of(t).wait())
    put_mat.wait()


def prepare(far_tile, far_count, far_w, band_w, seed_rows, labels):
    tiles, _, rows, _ = band_w.shape
    classes = labels.shape[1]
    total = far_tile.shape[0]
    chunks = tiles + total // CAP
    table = -(-(chunks * CAP + chunks + 1) // 128) * 128
    return pl.pallas_call(
        prep_kernel,
        out_shape=(
            jax.ShapeDtypeStruct((table,), jnp.int32),
            pltpu.HBM((chunks, rows, CAP * far_w.shape[1]), BF16),
            jax.ShapeDtypeStruct((rows, rows), F32),
            jax.ShapeDtypeStruct((2, rows, rows), BF16),
            pltpu.HBM((tiles, rows, classes), F32),
        ),
        in_specs=[SMEM, SMEM, VMEM, VMEM, ANY, ANY],
        out_specs=(SMEM, ANY, VMEM, VMEM, ANY),
        scratch_shapes=[
            pltpu.SMEM((chunks,), jnp.int32),
            pltpu.SMEM((chunks,), jnp.int32),
            pltpu.VMEM(band_w.shape, BF16),
            pltpu.VMEM(labels.shape, BF16),
            pltpu.VMEM((tiles, rows, classes), F32),
            pltpu.VMEM((tiles, rows, rows), F32),
            pltpu.VMEM((chunks, rows, CAP * far_w.shape[1]), BF16),
            DMA((2,)),
            DMA((tiles,)),
            DMA,
        ],
        cost_estimate=pl.CostEstimate(flops=10_000_000_000, bytes_accessed=16_000_000, transcendentals=0),
        compiler_params=pltpu.CompilerParams(vmem_limit_bytes=32 * MIB),
        name="prep",
    )(far_tile, far_count, seed_rows, far_w, in_hbm(band_w), in_hbm(labels))


def band_kernel(aux_ref, band_hbm, cur_hbm, old_hbm, base_hbm, res_ref, band_ref, cur_ref, old_ref, out_ref, part_ref, in_sem, out_sem):
    tiles, _, rows, _ = band_ref.shape
    gets = [
        pltpu.make_async_copy(src, dst, in_sem.at[i])
        for i, (src, dst) in enumerate(((band_hbm, band_ref), (cur_hbm, cur_ref), (old_hbm, old_ref)))
    ]
    for get in gets:
        get.start()
    part_ref[...] = jnp.zeros_like(part_ref)
    lane = lax.broadcasted_iota(jnp.int32, (rows, rows), 1)
    for get in gets:
        get.wait()

    def copy_of(t):
        return pltpu.make_async_copy(out_ref.at[t], base_hbm.at[t], out_sem.at[t])

    def step(t):
        place = pl.ds(pl.multiple_of(t * rows, rows), rows)
        here = cur_ref[place, :].astype(F32)
        seed = jnp.sum(jnp.where(lane == t, aux_ref[...], 0.0), axis=1, keepdims=True) < 0.0
        out_ref[t] = jnp.where(seed, here, band_sum(band_ref, cur_ref, t, tiles, rows))
        copy_of(t).start()
        gap = jnp.abs(here - old_ref[place, :].astype(F32))
        part_ref[pl.ds(t, 1), :] = fold(jnp.sum(gap, axis=0, keepdims=True), rows)

    step(0)
    loop(1, tiles - 1, step)
    step(tiles - 1)
    res_ref[...] = jnp.sum(part_ref[...].T, axis=0, keepdims=True)
    loop(0, tiles, lambda t: copy_of(t).wait())


def band_sums(aux, band_w, current, old):
    tiles, _, rows, _ = band_w.shape
    classes = current.shape[1]
    return pl.pallas_call(
        band_kernel,
        out_shape=(pltpu.HBM((tiles, rows, classes), F32), jax.ShapeDtypeStruct((1, rows), F32)),
        in_specs=[VMEM, ANY, ANY, ANY],
        out_specs=(ANY, VMEM),
        scratch_shapes=[
            pltpu.VMEM(band_w.shape, BF16),
            pltpu.VMEM(current.shape, BF16),
            pltpu.VMEM(current.shape, BF16),
            pltpu.VMEM((tiles, rows, classes), F32),
            pltpu.VMEM((rows, rows), F32),
            DMA((3,)),
            DMA((tiles,)),
        ],
        cost_estimate=pl.CostEstimate(flops=10_000_000_000, bytes_accessed=16_000_000, transcendentals=0),
        compiler_params=pltpu.CompilerParams(vmem_limit_bytes=32 * MIB),
        name="band",
    )(aux, in_hbm(band_w), in_hbm(current), in_hbm(old))


def far_kernel(first, *refs):
    if first:
        (table_ref, req_ref, aux_ref, low_ref, high_ref, edge_ref, recv_ref, mat_hbm, base_hbm,
         new_hbm, send_hbm, top_ref, end_ref,
         mat_ref, base_ref, new_ref, in_sem, rest_sem, out_sem, send_ref, send_sem) = refs
    else:
        (table_ref, res_ref, aux_ref, low_ref, high_ref, edge_ref, recv_ref, mat_hbm, base_hbm, cur_hbm,
         new_hbm, both_ref,
         mat_ref, base_ref, new_ref, in_sem, rest_sem, out_sem, cur_ref, part_ref) = refs
    tiles, rows, classes = base_ref.shape
    chunks = mat_ref.shape[0]
    num_at, ext_at, used_at = chunks * CAP, chunks * CAP + tiles, chunks * CAP + chunks
    block = new_ref.shape[1]
    per = rows // block

    def group_copies(g):
        here = pl.ds(g * GROUP, GROUP)
        copies = [
            pltpu.make_async_copy(mat_hbm.at[here], mat_ref.at[here], in_sem.at[0, g]),
            pltpu.make_async_copy(base_hbm.at[here], base_ref.at[here], in_sem.at[1, g]),
        ]
        if not first:
            wide = pl.ds(g * GROUP * per, GROUP * per)
            copies.append(pltpu.make_async_copy(cur_hbm.at[wide], cur_ref.at[wide], in_sem.at[2, g]))
        return copies

    groups = tiles // GROUP
    for g in range(groups):
        for copy in group_copies(g):
            copy.start()
    rest = pl.ds(tiles, chunks - tiles)
    get_rest = pltpu.make_async_copy(mat_hbm.at[rest], mat_ref.at[rest], rest_sem)

    @pl.when(table_ref[used_at] > 0)
    def _():
        get_rest.start()
        get_rest.wait()

    if not first:
        part_ref[...] = jnp.zeros_like(part_ref)
    lane = lax.broadcasted_iota(jnp.int32, (rows, rows), 1)

    def gathered(c):
        parts = [recv_ref[table_ref[c * CAP + p]].astype(F32) for p in range(CAP)]
        return jnp.concatenate(parts, axis=0).astype(BF16)

    def out_copy(t):
        here = pl.ds(t * per, per)
        return pltpu.make_async_copy(new_ref.at[here], new_hbm.at[here], out_sem.at[t])

    def use(t, acc):
        here = pl.ds(t * per, per)
        signed = jnp.sum(jnp.where(lane == t, aux_ref[...], 0.0), axis=1, keepdims=True)
        mean = jnp.sum(acc * acc, axis=1, keepdims=True) * (1.0 / classes)
        scale = jnp.where(signed < 0.0, 1.0, signed / jnp.maximum(signed * jnp.sqrt(mean), 0.05))
        fresh = (acc * scale).astype(BF16)
        new_ref[here] = fresh.astype(F32).reshape(per, block, classes).astype(BF16)
        if not first:
            gap = jnp.abs(fresh.astype(F32) - cur_ref[here].astype(F32).reshape(rows, classes))
            part_ref[pl.ds(t, 1), :] = fold(jnp.sum(gap, axis=0, keepdims=True), rows)

    def tile_step(t):
        use(t, base_ref[t] + dot(mat_ref[t], gathered(t)))
        out_copy(t).start()

    def group_step(g):
        for copy in group_copies(g):
            copy.wait()

        @pl.when(g == 0)
        def _():
            base_ref[0] += dot(edge_ref[0], low_ref[...])

        @pl.when(g == groups - 1)
        def _():
            base_ref[tiles - 1] += dot(edge_ref[1], high_ref[...])

        def extra(c):
            t = table_ref[ext_at + c]

            @pl.when(lax.div(t, GROUP) == g)
            def _():
                base_ref[t] += dot(mat_ref[tiles + c], gathered(tiles + c))

        loop(0, table_ref[used_at], extra)
        for i in range(GROUP):
            tile_step(g * GROUP + i)

    loop(0, groups, group_step)
    if first:
        peers = req_ref.shape[1]
        parts = send_sem.shape[0]
        share = peers // parts

        def send_copy(part):
            here = pl.ds(part * share * req_ref.shape[0], share * req_ref.shape[0])
            return pltpu.make_async_copy(send_ref.at[here], send_hbm.at[here], send_sem.at[part])

        def choose(d):
            for k in range(req_ref.shape[0]):
                send_ref[d * req_ref.shape[0] + k] = new_ref[req_ref[k, d]]

        for part in range(parts):
            loop(part * share, (part + 1) * share, choose, unroll=8)
            send_copy(part).start()
        top_ref[...] = new_ref[0:per]
        end_ref[...] = new_ref[(tiles - 1) * per :]
        for part in range(parts):
            send_copy(part).wait()
    else:
        last = jnp.sum(part_ref[...].T, axis=0, keepdims=True)
        both_ref[0:1, :] = res_ref[:, :tiles]
        both_ref[1:2, :] = last[:, :tiles]
    loop(0, tiles, lambda t: out_copy(t).wait())


def far_call(first, args, tiles, rows, classes, chunks, total, block):
    blocks = pltpu.HBM((tiles * rows // block, block, classes), BF16)
    half = jax.ShapeDtypeStruct((rows // block, block, classes), BF16)
    picked = pltpu.HBM((total, block, classes), BF16)
    scratch = [
        pltpu.VMEM((chunks, rows, CAP * block), BF16),
        pltpu.VMEM((tiles, rows, classes), F32),
        pltpu.VMEM(blocks.shape, BF16),
        DMA((3, tiles // GROUP)),
        DMA,
        DMA((tiles,)),
    ]
    if first:
        outs, specs = (blocks, picked, half, half), (ANY, ANY, VMEM, VMEM)
        ins = [SMEM, SMEM] + [VMEM] * 5 + [ANY] * 2
        scratch += [pltpu.VMEM(picked.shape, BF16), DMA((4,))]
    else:
        outs, specs = (blocks, jax.ShapeDtypeStruct((ITERS, tiles), F32)), (ANY, VMEM)
        ins = [SMEM] + [VMEM] * 6 + [ANY] * 3
        scratch += [pltpu.VMEM(blocks.shape, BF16), pltpu.VMEM((rows, rows), F32)]
    return pl.pallas_call(
        lambda *refs: far_kernel(first, *refs),
        out_shape=outs,
        in_specs=ins,
        out_specs=specs,
        scratch_shapes=scratch,
        cost_estimate=pl.CostEstimate(flops=4_000_000_000, bytes_accessed=18_000_000, transcendentals=0),
        compiler_params=pltpu.CompilerParams(vmem_limit_bytes=32 * MIB),
        name="far_first" if first else "far_last",
    )(*args)


def halos(first, last):
    count = lax.axis_size("node")
    forward = [(i, (i + 1) % count) for i in range(count)]
    backward = [(target, source) for source, target in forward]
    return lax.ppermute(last, "node", forward), lax.ppermute(first, "node", backward)


def body(labels, seed_mask, band_w, far_block, far_tile, far_count, far_w):
    node_rows, classes = labels.shape
    tiles, _, rows, _ = band_w.shape
    _, peers, slots, block, _ = far_w.shape
    total = peers * slots
    got = lax.all_to_all(far_block, "node", split_axis=1, concat_axis=0, tiled=True)
    blocks = labels.reshape(-1, block, classes)
    requests, send = pick_blocks(got, blocks)

    def exchange(x):
        x = x.reshape(peers, slots, block, classes)
        return lax.all_to_all(x, "node", split_axis=0, concat_axis=0, tiled=True).reshape(total, block, classes)

    recv = exchange(send)
    low, high = halos(labels[:rows], labels[-rows:])
    table, mat, aux, edges, base = prepare(
        far_tile[0].T.reshape(total), far_count[0], far_w.reshape(total, block, rows), band_w,
        seed_mask.reshape(tiles, 1, rows), labels,
    )
    sizes = (tiles, rows, classes, mat.shape[0], total, block)
    new, send, top, end = far_call(True, (table, requests, aux, low, high, edges, in_vmem(recv), in_hbm(mat), in_hbm(base)), *sizes)
    recv = exchange(send)
    low, high = halos(top.reshape(rows, classes), end.reshape(rows, classes))
    base, change = band_sums(aux, band_w, new.reshape(node_rows, classes), labels)
    final, both = far_call(False, (table, change, aux, low, high, edges, in_vmem(recv), in_hbm(mat), in_hbm(base), in_hbm(new)), *sizes)
    return final.reshape(node_rows, classes), both


def solution(mesh):
    placed = (
        P("node", None),
        P("node"),
        P("node", None, None, None),
        P("node", None, None),
        P("node", None, None),
        P("node", None),
        P("node", None, None, None, None),
    )
    return jax.shard_map(
        body,
        mesh=mesh,
        in_specs=placed,
        out_specs=(P("node", None), P(None, "node")),
        check_vma=False,
    )
```

```python
import jax
import jax.numpy as jnp
from jax import lax
from jax.experimental import pallas as pl
from jax.experimental.pallas import tpu as pltpu
from jax.sharding import PartitionSpec as P

ITERS = 2
CAP = 16
GROUP = 4
AHEAD = 4
UNROLL = 8
F32 = jnp.float32
BF16 = jnp.bfloat16
VMEM = pl.BlockSpec(memory_space=pltpu.VMEM)
SMEM = pl.BlockSpec(memory_space=pltpu.SMEM)
ANY = pl.BlockSpec(memory_space=pltpu.HBM)
MIB = 1 << 20
DMA = pltpu.SemaphoreType.DMA


def in_hbm(x):
    return pltpu.with_memory_space_constraint(x, pltpu.HBM)


def in_vmem(x):
    return pltpu.with_memory_space_constraint(x, pltpu.VMEM)


def dot(a, b):
    return jnp.dot(a, b, preferred_element_type=F32)


def loop(low, high, step, unroll=1):
    def run(i, carry):
        step(i)
        return carry

    lax.fori_loop(low, high, run, 0, unroll=unroll)


def gap_sum(new, old, shape):
    gap = jnp.abs(new - old).astype(F32)
    total = jnp.zeros(shape, F32)
    for j in range(gap.shape[1] // shape[1]):
        column = gap[:, j * shape[1] : (j + 1) * shape[1]]
        total = total + jnp.sum(column.reshape(-1, *shape), axis=0)
    return total


def lane_totals(parts):
    sums = jnp.sum(parts, axis=1)
    tiles, lanes = sums.shape
    square = jnp.concatenate([sums, jnp.zeros((lanes - tiles, lanes), F32)], axis=0)
    return jnp.sum(square.T, axis=0, keepdims=True)


def pick_kernel(got_ref, cur_ref, req_ref, send_ref, flat_ref, held_ref, word_sem, in_sem, out_sem):
    slots, peers = req_ref.shape
    table = jnp.concatenate([got_ref[:, 0, :], jnp.zeros((peers, peers - slots), jnp.int32)], axis=1)
    flat_ref[...] = table.T[:8, :]
    move = pltpu.make_async_copy(flat_ref.at[pl.ds(0, slots)], req_ref, word_sem)
    move.start()
    move.wait()
    parts = in_sem.shape[0]
    batch = held_ref.shape[1] // slots
    share = held_ref.shape[0] // parts

    def fetch(i, part):
        for j in range(batch):
            for k in range(slots):
                row = req_ref[k, i * batch + j]
                pltpu.make_async_copy(cur_ref.at[row], held_ref.at[i, j * slots + k], in_sem.at[part]).start()

    for part in range(parts):
        loop(part * share, (part + 1) * share, lambda i: fetch(i, part))
    for part in range(parts):
        here = pl.ds(part * share, share)
        pltpu.make_async_copy(held_ref.at[here], held_ref.at[here], in_sem.at[part]).wait()
        pltpu.make_async_copy(held_ref.at[here], send_ref.at[here], out_sem.at[part]).start()
    for part in range(parts):
        here = pl.ds(part * share, share)
        pltpu.make_async_copy(held_ref.at[here], send_ref.at[here], out_sem.at[part]).wait()


def pick_blocks(got, blocks):
    peers, _, slots = got.shape
    shape = (peers * slots // CAP, CAP) + blocks.shape[1:]
    return pl.pallas_call(
        pick_kernel,
        out_shape=(jax.ShapeDtypeStruct((slots, peers), jnp.int32), pltpu.HBM(shape, BF16)),
        in_specs=[VMEM, ANY],
        out_specs=(SMEM, ANY),
        scratch_shapes=[pltpu.VMEM((8, peers), jnp.int32), pltpu.VMEM(shape, BF16), DMA, DMA((4,)), DMA((4,))],
        cost_estimate=pl.CostEstimate(flops=1_000_000_000, bytes_accessed=4_000_000, transcendentals=0),
        compiler_params=pltpu.CompilerParams(vmem_limit_bytes=32 * MIB),
        name="pick",
    )(in_vmem(got), in_hbm(blocks))


def prep_kernel(
    tile_ref, count_ref, seed_ref, far_ref, band_hbm,
    table_ref, aux_ref, wide_hbm, more_hbm,
    cnt_ref, num_ref, band_ref, wide_ref, more_ref, deg_ref, in_sem, out_sem, more_sem,
):
    peers = count_ref.shape[0]
    total = tile_ref.shape[0]
    slots = total // peers
    tiles, _, rows, _ = band_ref.shape
    chunks = tiles + more_ref.shape[0]
    ext_at, used_at = chunks * CAP, chunks * CAP + more_ref.shape[0]
    get_band = pltpu.make_async_copy(band_hbm, band_ref, in_sem)
    get_band.start()

    def clear(i):
        table_ref[i] = 0

    loop(0, table_ref.shape[0], clear, unroll=16)

    def clear_count(i):
        cnt_ref[i] = 0
        num_ref[i] = 0

    loop(0, chunks, clear_count, unroll=8)

    def scan(peer):
        live = count_ref[peer]
        for k in range(slots):
            @pl.when(k < live)
            def _():
                tile = tile_ref[k * peers + peer]
                place = num_ref[tile]
                num_ref[tile] = place + 1
                slot = peer * slots + k

                @pl.when(place < CAP)
                def _():
                    table_ref[tile * CAP + place] = slot

                @pl.when(place >= CAP)
                def _():
                    inner = lax.rem(place, CAP)

                    @pl.when(inner == 0)
                    def _():
                        fresh = table_ref[used_at]
                        table_ref[ext_at + fresh] = tile
                        table_ref[used_at] = fresh + 1

                    def find(c, last):
                        return jnp.where(table_ref[ext_at + c] == tile, c, last)

                    chunk = tiles + lax.fori_loop(0, table_ref[used_at], find, 0)
                    table_ref[chunk * CAP + inner] = slot
                    cnt_ref[chunk] = inner + 1

    loop(0, peers, scan, unroll=2)

    def tidy(t):
        cnt_ref[t] = jnp.minimum(num_ref[t], CAP)

    loop(0, tiles, tidy)

    def seeded(t):
        return jnp.broadcast_to(seed_ref[t].astype(F32), (rows, rows)).T == 1.0

    def weights(c):
        parts = [far_ref[table_ref[c * CAP + p]].astype(F32) for p in range(CAP)]
        mat = jnp.concatenate(parts, axis=0)
        depth = lax.broadcasted_iota(jnp.int32, mat.shape, 0)
        return jnp.where(depth < cnt_ref[c] * far_ref.shape[1], mat, 0.0).T

    get_band.wait()
    groups = tiles // GROUP

    def put_wide(g):
        here = pl.ds(g * GROUP, GROUP)
        return pltpu.make_async_copy(wide_ref.at[here], wide_hbm.at[here], out_sem.at[g])

    lane = lax.broadcasted_iota(jnp.int32, (rows, rows), 1)
    eye = (lane == lax.broadcasted_iota(jnp.int32, (rows, rows), 0)).astype(F32)

    def tile_step(t):
        seed = seeded(t)
        near = [band_ref[t, o].astype(F32) for o in range(3)]
        far = weights(t)
        degree = jnp.sum(near[0] + near[1] + near[2] + far, axis=1, keepdims=True)
        deg_ref[t] = jnp.broadcast_to(degree, (rows, rows))
        for j, (kept, other) in enumerate(zip(near + [far], (0.0, eye, 0.0, 0.0))):
            wide_ref[t, :, j * rows : (j + 1) * rows] = jnp.where(seed, other, kept).astype(BF16)

    def group_step(g):
        for i in range(GROUP):
            tile_step(g * GROUP + i)
        put_wide(g).start()

    loop(0, groups, group_step)

    def extra_step(c):
        t = table_ref[ext_at + c]
        mat = weights(tiles + c)
        more_ref[c] = jnp.where(seeded(t), 0.0, mat).astype(BF16)
        deg_ref[t] = deg_ref[t] + jnp.sum(mat, axis=1, keepdims=True)

    loop(0, table_ref[used_at], extra_step)
    put_more = pltpu.make_async_copy(more_ref, more_hbm, more_sem)
    put_more.start()
    aux_ref[...] = jnp.ones_like(aux_ref)

    def finish(t):
        cap = 1.0 / deg_ref[t] / 0.05
        aux_ref[...] = jnp.where(lane == t, jnp.where(seeded(t), -1.0, cap), aux_ref[...])

    loop(0, tiles, finish, unroll=2)
    loop(0, groups, lambda g: put_wide(g).wait())
    put_more.wait()


def prepare(far_tile, far_count, far_w, band_w, seed_rows):
    tiles, _, rows, _ = band_w.shape
    total = far_tile.shape[0]
    extra = total // CAP
    depth = CAP * far_w.shape[1]
    table = -(-((tiles + extra) * CAP + extra + 1) // 128) * 128
    wide = (tiles, rows, 3 * rows + depth)
    more = (extra, rows, depth)
    return pl.pallas_call(
        prep_kernel,
        out_shape=(
            jax.ShapeDtypeStruct((table,), jnp.int32),
            jax.ShapeDtypeStruct((rows, rows), F32),
            pltpu.HBM(wide, BF16),
            pltpu.HBM(more, BF16),
        ),
        in_specs=[SMEM, SMEM, VMEM, VMEM, ANY],
        out_specs=(SMEM, VMEM, ANY, ANY),
        scratch_shapes=[
            pltpu.SMEM((tiles + extra,), jnp.int32),
            pltpu.SMEM((tiles + extra,), jnp.int32),
            pltpu.VMEM(band_w.shape, BF16),
            pltpu.VMEM(wide, BF16),
            pltpu.VMEM(more, BF16),
            pltpu.VMEM((tiles, rows, rows), F32),
            DMA,
            DMA((tiles // GROUP,)),
            DMA,
        ],
        cost_estimate=pl.CostEstimate(flops=10_000_000_000, bytes_accessed=16_000_000, transcendentals=0),
        compiler_params=pltpu.CompilerParams(vmem_limit_bytes=32 * MIB),
        name="prep",
    )(far_tile, far_count, seed_rows, far_w, in_hbm(band_w))


def change_kernel(cur_hbm, old_hbm, res_ref, cur_ref, old_ref, part_ref, sem):
    groups = sem.shape[1]
    rows = cur_ref.shape[0] // part_ref.shape[0]
    span = cur_ref.shape[0] // groups

    def copies(g):
        here = pl.ds(g * span, span)
        return (
            pltpu.make_async_copy(cur_hbm.at[here], cur_ref.at[here], sem.at[0, g]),
            pltpu.make_async_copy(old_hbm.at[here], old_ref.at[here], sem.at[1, g]),
        )

    for g in range(groups):
        for copy in copies(g):
            copy.start()

    def step(g):
        for copy in copies(g):
            copy.wait()

        def tile(t):
            place = pl.ds(pl.multiple_of(t * rows, rows), rows)
            part_ref[t] = gap_sum(cur_ref[place, :], old_ref[place, :], part_ref.shape[1:])

        loop(g * (span // rows), (g + 1) * (span // rows), tile)

    loop(0, groups, step)
    res_ref[...] = lane_totals(part_ref[...])


def change_sums(current, old, rows, groups):
    return pl.pallas_call(
        change_kernel,
        out_shape=jax.ShapeDtypeStruct((1, rows), F32),
        in_specs=[ANY, ANY],
        out_specs=VMEM,
        scratch_shapes=[
            pltpu.VMEM(current.shape, BF16),
            pltpu.VMEM(current.shape, BF16),
            pltpu.VMEM((current.shape[0] // rows, 8, rows), F32),
            DMA((2, groups)),
        ],
        cost_estimate=pl.CostEstimate(flops=5_000_000_000, bytes_accessed=8_000_000, transcendentals=0),
        compiler_params=pltpu.CompilerParams(vmem_limit_bytes=32 * MIB),
        name="change",
    )(in_hbm(current), in_hbm(old))


def spread_kernel(first, *refs):
    if first:
        (table_ref, req_ref, aux_ref, low_ref, high_ref, recv_ref, wide_hbm, more_hbm, cur_hbm,
         new_hbm, send_hbm, top_ref, end_ref,
         wide_ref, more_ref, cur_ref, new_ref, far_ref, in_sem, more_sem, out_sem, send_ref, send_sem) = refs
    else:
        (table_ref, res_ref, aux_ref, low_ref, high_ref, recv_ref, wide_hbm, more_hbm, cur_hbm,
         new_hbm, both_ref,
         wide_ref, more_ref, cur_ref, new_ref, far_ref, in_sem, more_sem, out_sem, part_ref) = refs
    tiles, rows, width = wide_ref.shape
    extra = more_ref.shape[0]
    classes = cur_ref.shape[1]
    ext_at, used_at = (tiles + extra) * CAP, (tiles + extra) * CAP + extra
    block = new_ref.shape[1]
    per = rows // block
    groups = tiles // GROUP
    span = GROUP * rows

    def get_cur(g):
        start = pl.multiple_of(g * span, span)
        return pltpu.make_async_copy(cur_hbm.at[pl.ds(start, span)], cur_ref.at[pl.ds(start + rows, span)], in_sem.at[0, g])

    def get_wide(g):
        here = pl.ds(g * GROUP, GROUP)
        return pltpu.make_async_copy(wide_hbm.at[here], wide_ref.at[here], in_sem.at[1, g])

    def fetch(g):
        get_wide(g).start()

        @pl.when(g + 1 < groups)
        def _():
            get_cur(g + 1).start()

    get_cur(0).start()
    for g in range(AHEAD):
        fetch(g)
    get_more = pltpu.make_async_copy(more_hbm, more_ref, more_sem)

    @pl.when(table_ref[used_at] > 0)
    def _():
        get_more.start()
        get_more.wait()

    cur_ref[0:rows, :] = low_ref[...]
    cur_ref[(tiles + 1) * rows :, :] = high_ref[...]
    lane = lax.broadcasted_iota(jnp.int32, (rows, rows), 1)

    def gathered(c):
        parts = [recv_ref[table_ref[c * CAP + p]].astype(F32) for p in range(CAP)]
        return jnp.concatenate(parts, axis=0).astype(BF16)

    def put_new(g):
        here = pl.ds(g * GROUP * per, GROUP * per)
        return pltpu.make_async_copy(new_ref.at[here], new_hbm.at[here], out_sem.at[g])

    def total(t):
        near = cur_ref[pl.ds(pl.multiple_of(t * rows, rows), 3 * rows), :]
        return dot(wide_ref[t], jnp.concatenate([near, far_ref[t]], axis=0))

    def finish(t, acc):
        cap = jnp.sum(jnp.where(lane == t, aux_ref[...], 0.0), axis=1, keepdims=True)
        mean = jnp.sum(acc * acc, axis=1, keepdims=True) * (1.0 / classes)
        scale = jnp.where(cap < 0.0, 1.0, jnp.minimum(lax.rsqrt(mean), cap))
        fresh = acc * scale
        here = pl.ds(t * per, per)
        if first:
            new_ref[here] = fresh.reshape(per, block, classes).astype(BF16)
        else:
            new_ref[here] = fresh.reshape(per, block, classes).astype(BF16)
            old = cur_ref[pl.ds(pl.multiple_of((t + 1) * rows, rows), rows), :]
            part_ref[t] = gap_sum(fresh.astype(BF16), old, part_ref.shape[1:])

    def patch(t, used):
        acc = total(t)

        def add(c, acc):
            part = dot(more_ref[c], gathered(tiles + c))
            return acc + jnp.where(table_ref[ext_at + c] == t, part, 0.0)

        finish(t, lax.fori_loop(0, used, add, acc))

    def place(t):
        far_ref[t] = gathered(t)

    loop(0, tiles, place, unroll=2)
    get_cur(0).wait()

    def ready(g):
        @pl.when(g + AHEAD < groups)
        def _():
            fetch(g + AHEAD)

        get_wide(g).wait()

        @pl.when(g + 1 < groups)
        def _():
            get_cur(g + 1).wait()

    def big_step(b):
        for i in range(UNROLL // GROUP):
            ready(b * (UNROLL // GROUP) + i)

        def count(c, found):
            return found + jnp.where(lax.div(table_ref[ext_at + c], UNROLL) == b, 1, 0)

        used = table_ref[used_at]
        heavy = lax.fori_loop(0, used, count, 0) > 0

        @pl.when(jnp.logical_not(heavy))
        def _():
            for i in range(UNROLL):
                finish(b * UNROLL + i, total(b * UNROLL + i))

        @pl.when(heavy)
        def _():
            loop(b * UNROLL, (b + 1) * UNROLL, lambda t: patch(t, used))

        for i in range(UNROLL // GROUP):
            put_new(b * (UNROLL // GROUP) + i).start()

    loop(0, tiles // UNROLL, big_step)
    if first:
        slots = req_ref.shape[0]
        parts = send_sem.shape[0]
        batch = send_ref.shape[1]
        share = send_ref.shape[0] // parts

        def send_copy(part):
            here = pl.ds(part * share, share)
            return pltpu.make_async_copy(send_ref.at[here], send_hbm.at[here], send_sem.at[part])

        def choose(i):
            for j in range(batch):
                send_ref[i, j] = new_ref[req_ref[j % slots, i * (batch // slots) + j // slots]]

        for part in range(parts):
            loop(part * share, (part + 1) * share, choose)
            send_copy(part).start()
        top_ref[...] = new_ref[0:per]
        end_ref[...] = new_ref[(tiles - 1) * per :]
        for part in range(parts):
            send_copy(part).wait()
    else:
        both_ref[0:1, :] = res_ref[:, :tiles]
        both_ref[1:2, :] = lane_totals(part_ref[...])[:, :tiles]
    loop(0, groups, lambda g: put_new(g).wait())


def spread_call(first, table, side, aux, low, high, recv, wide, more, current):
    tiles, rows, _ = wide.shape
    total, block, classes = recv.shape
    blocks = pltpu.HBM((tiles * rows // block, block, classes), BF16)
    half = jax.ShapeDtypeStruct((rows // block, block, classes), BF16)
    picked = pltpu.HBM((total // CAP, CAP, block, classes), BF16)
    scratch = [
        pltpu.VMEM(wide.shape, BF16),
        pltpu.VMEM(more.shape, BF16),
        pltpu.VMEM(((tiles + 2) * rows, classes), BF16),
        pltpu.VMEM(blocks.shape, BF16),
        pltpu.VMEM((tiles, CAP * block, classes), BF16),
        DMA((2, tiles // GROUP)),
        DMA,
        DMA((tiles // GROUP,)),
    ]
    if first:
        outs, specs = (blocks, picked, half, half), (ANY, ANY, VMEM, VMEM)
        scratch += [pltpu.VMEM(picked.shape, BF16), DMA((4,))]
    else:
        outs, specs = (blocks, jax.ShapeDtypeStruct((ITERS, tiles), F32)), (ANY, VMEM)
        scratch += [pltpu.VMEM((tiles, 8, rows), F32)]
    return pl.pallas_call(
        lambda *refs: spread_kernel(first, *refs),
        out_shape=outs,
        in_specs=[SMEM, SMEM if first else VMEM] + [VMEM] * 4 + [ANY] * 3,
        out_specs=specs,
        scratch_shapes=scratch,
        cost_estimate=pl.CostEstimate(flops=4_000_000_000, bytes_accessed=18_000_000, transcendentals=0),
        compiler_params=pltpu.CompilerParams(vmem_limit_bytes=32 * MIB),
        name="spread_first" if first else "spread_last",
    )(table, side, aux, low, high, in_vmem(recv), in_hbm(wide), in_hbm(more), in_hbm(current))


def halos(first, last):
    count = lax.axis_size("node")
    forward = [(i, (i + 1) % count) for i in range(count)]
    backward = [(target, source) for source, target in forward]
    return lax.ppermute(last, "node", forward), lax.ppermute(first, "node", backward)


def body(labels, seed_mask, band_w, far_block, far_tile, far_count, far_w):
    node_rows, classes = labels.shape
    tiles, _, rows, _ = band_w.shape
    _, peers, slots, block, _ = far_w.shape
    total = peers * slots
    got = lax.all_to_all(far_block, "node", split_axis=1, concat_axis=0, tiled=True)
    blocks = labels.reshape(-1, block, classes)
    requests, send = pick_blocks(got, blocks)

    def exchange(x):
        x = x.reshape(peers, slots, block, classes)
        return lax.all_to_all(x, "node", split_axis=0, concat_axis=0, tiled=True).reshape(total, block, classes)

    recv = exchange(send)
    low, high = halos(labels[:rows], labels[-rows:])
    table, aux, wide, more = prepare(
        far_tile[0].T.reshape(total), far_count[0], far_w.reshape(total, block, rows), band_w, seed_mask.reshape(tiles, 1, rows)
    )
    new, send, top, end = spread_call(True, table, requests, aux, low, high, recv, wide, more, labels)
    recv = exchange(send)
    low, high = halos(top.reshape(rows, classes), end.reshape(rows, classes))
    current = new.reshape(node_rows, classes)
    change = change_sums(current, labels, rows, tiles // GROUP)
    final, both = spread_call(False, table, change, aux, low, high, recv, wide, more, current)
    return final.reshape(node_rows, classes), both


def solution(mesh):
    placed = (
        P("node", None),
        P("node"),
        P("node", None, None, None),
        P("node", None, None),
        P("node", None, None),
        P("node", None),
        P("node", None, None, None, None),
    )
    return jax.shard_map(
        body,
        mesh=mesh,
        in_specs=placed,
        out_specs=(P("node", None), P(None, "node")),
        check_vma=False,
    )
```

```python
import jax
import jax.numpy as jnp
from jax import lax
from jax.experimental import pallas as pl
from jax.experimental.pallas import tpu as pltpu
from jax.sharding import PartitionSpec as P

ITERS = 2
CAP = 16
GROUP = 4
AHEAD = 4
UNROLL = 8
F32 = jnp.float32
BF16 = jnp.bfloat16
VMEM = pl.BlockSpec(memory_space=pltpu.VMEM)
SMEM = pl.BlockSpec(memory_space=pltpu.SMEM)
ANY = pl.BlockSpec(memory_space=pltpu.HBM)
MIB = 1 << 20
DMA = pltpu.SemaphoreType.DMA


def in_hbm(x):
    return pltpu.with_memory_space_constraint(x, pltpu.HBM)


def in_vmem(x):
    return pltpu.with_memory_space_constraint(x, pltpu.VMEM)


def dot(a, b):
    return jnp.dot(a, b, preferred_element_type=F32)


def loop(low, high, step, unroll=1):
    def run(i, carry):
        step(i)
        return carry

    lax.fori_loop(low, high, run, 0, unroll=unroll)


def gap_sum(new, old, shape):
    gap = jnp.abs(new - old).astype(F32)
    total = jnp.zeros(shape, F32)
    for j in range(gap.shape[1] // shape[1]):
        column = gap[:, j * shape[1] : (j + 1) * shape[1]]
        total = total + jnp.sum(column.reshape(-1, *shape), axis=0)
    return total


def lane_totals(parts):
    sums = jnp.sum(parts, axis=1)
    tiles, lanes = sums.shape
    square = jnp.concatenate([sums, jnp.zeros((lanes - tiles, lanes), F32)], axis=0)
    return jnp.sum(square.T, axis=0, keepdims=True)


def pick_kernel(got_ref, cur_ref, req_hbm, send_ref, flat_ref, req_ref, held_ref, word_sem, in_sem, out_sem):
    slots, peers = req_ref.shape
    table = jnp.concatenate([got_ref[:, 0, :], jnp.zeros((peers, peers - slots), jnp.int32)], axis=1)
    flat_ref[...] = table.T[:8, :]
    move = pltpu.make_async_copy(flat_ref.at[pl.ds(0, slots)], req_ref, word_sem)
    move.start()
    move.wait()
    keep = pltpu.make_async_copy(req_ref, req_hbm, word_sem)
    keep.start()
    parts = in_sem.shape[0]
    batch = held_ref.shape[1] // slots
    share = held_ref.shape[0] // parts

    def fetch(i, part):
        for j in range(batch):
            for k in range(slots):
                row = req_ref[k, i * batch + j]
                pltpu.make_async_copy(cur_ref.at[row], held_ref.at[i, j * slots + k], in_sem.at[part]).start()

    for part in range(parts):
        loop(part * share, (part + 1) * share, lambda i: fetch(i, part))
    for part in range(parts):
        here = pl.ds(part * share, share)
        pltpu.make_async_copy(held_ref.at[here], held_ref.at[here], in_sem.at[part]).wait()
        pltpu.make_async_copy(held_ref.at[here], send_ref.at[here], out_sem.at[part]).start()
    for part in range(parts):
        here = pl.ds(part * share, share)
        pltpu.make_async_copy(held_ref.at[here], send_ref.at[here], out_sem.at[part]).wait()
    keep.wait()


def pick_blocks(got, blocks):
    peers, _, slots = got.shape
    shape = (peers * slots // CAP, CAP) + blocks.shape[1:]
    return pl.pallas_call(
        pick_kernel,
        out_shape=(pltpu.HBM((slots, peers), jnp.int32), pltpu.HBM(shape, BF16)),
        in_specs=[VMEM, ANY],
        out_specs=(ANY, ANY),
        scratch_shapes=[
            pltpu.VMEM((8, peers), jnp.int32),
            pltpu.SMEM((slots, peers), jnp.int32),
            pltpu.VMEM(shape, BF16),
            DMA,
            DMA((4,)),
            DMA((4,)),
        ],
        cost_estimate=pl.CostEstimate(flops=1_000_000_000, bytes_accessed=4_000_000, transcendentals=0),
        compiler_params=pltpu.CompilerParams(vmem_limit_bytes=32 * MIB),
        name="pick",
    )(in_vmem(got), in_hbm(blocks))


def prep_kernel(
    tile_ref, count_ref, seed_ref, far_ref, band_hbm,
    table_hbm, aux_ref, wide_hbm, more_hbm,
    table_ref, cnt_ref, num_ref, band_ref, wide_ref, more_ref, deg_ref, in_sem, out_sem, more_sem, table_sem,
):
    peers = count_ref.shape[0]
    total = tile_ref.shape[0]
    slots = total // peers
    tiles, _, rows, _ = band_ref.shape
    chunks = tiles + more_ref.shape[0]
    ext_at, used_at = chunks * CAP, chunks * CAP + more_ref.shape[0]
    get_band = pltpu.make_async_copy(band_hbm, band_ref, in_sem)
    get_band.start()

    def clear(i):
        table_ref[i] = 0

    loop(0, table_ref.shape[0], clear, unroll=16)

    def clear_count(i):
        cnt_ref[i] = 0
        num_ref[i] = 0

    loop(0, chunks, clear_count, unroll=8)

    def scan(peer):
        live = count_ref[peer]
        for k in range(slots):
            @pl.when(k < live)
            def _():
                tile = tile_ref[k * peers + peer]
                place = num_ref[tile]
                num_ref[tile] = place + 1
                slot = peer * slots + k

                @pl.when(place < CAP)
                def _():
                    table_ref[tile * CAP + place] = slot

                @pl.when(place >= CAP)
                def _():
                    inner = lax.rem(place, CAP)

                    @pl.when(inner == 0)
                    def _():
                        fresh = table_ref[used_at]
                        table_ref[ext_at + fresh] = tile
                        table_ref[used_at] = fresh + 1

                    def find(c, last):
                        return jnp.where(table_ref[ext_at + c] == tile, c, last)

                    chunk = tiles + lax.fori_loop(0, table_ref[used_at], find, 0)
                    table_ref[chunk * CAP + inner] = slot
                    cnt_ref[chunk] = inner + 1

    loop(0, peers, scan, unroll=2)

    put_table = pltpu.make_async_copy(table_ref, table_hbm, table_sem)
    put_table.start()

    def tidy(t):
        cnt_ref[t] = jnp.minimum(num_ref[t], CAP)

    loop(0, tiles, tidy)

    def seeded(t):
        return jnp.broadcast_to(seed_ref[t].astype(F32), (rows, rows)).T == 1.0

    def weights(c):
        parts = [far_ref[table_ref[c * CAP + p]].astype(F32) for p in range(CAP)]
        mat = jnp.concatenate(parts, axis=0)
        depth = lax.broadcasted_iota(jnp.int32, mat.shape, 0)
        return jnp.where(depth < cnt_ref[c] * far_ref.shape[1], mat, 0.0).T

    get_band.wait()
    groups = tiles // GROUP

    def put_wide(g):
        here = pl.ds(g * GROUP, GROUP)
        return pltpu.make_async_copy(wide_ref.at[here], wide_hbm.at[here], out_sem.at[g])

    lane = lax.broadcasted_iota(jnp.int32, (rows, rows), 1)
    eye = (lane == lax.broadcasted_iota(jnp.int32, (rows, rows), 0)).astype(F32)

    def tile_step(t):
        seed = seeded(t)
        near = [band_ref[t, o].astype(F32) for o in range(3)]
        far = weights(t)
        degree = jnp.sum(near[0] + near[1] + near[2] + far, axis=1, keepdims=True)
        deg_ref[t] = jnp.broadcast_to(degree, (rows, rows))
        for j, (kept, other) in enumerate(zip(near + [far], (0.0, eye, 0.0, 0.0))):
            wide_ref[t, :, j * rows : (j + 1) * rows] = jnp.where(seed, other, kept).astype(BF16)

    def group_step(g):
        for i in range(GROUP):
            tile_step(g * GROUP + i)
        put_wide(g).start()

    loop(0, groups, group_step)

    def extra_step(c):
        t = table_ref[ext_at + c]
        mat = weights(tiles + c)
        more_ref[c] = jnp.where(seeded(t), 0.0, mat).astype(BF16)
        deg_ref[t] = deg_ref[t] + jnp.sum(mat, axis=1, keepdims=True)

    loop(0, table_ref[used_at], extra_step)
    put_more = pltpu.make_async_copy(more_ref, more_hbm, more_sem)
    put_more.start()
    aux_ref[...] = jnp.ones_like(aux_ref)

    def finish(t):
        cap = 1.0 / deg_ref[t] / 0.05
        aux_ref[...] = jnp.where(lane == t, jnp.where(seeded(t), -1.0, cap), aux_ref[...])

    loop(0, tiles, finish, unroll=2)
    loop(0, groups, lambda g: put_wide(g).wait())
    put_more.wait()
    put_table.wait()


def prepare(far_tile, far_count, far_w, band_w, seed_rows):
    tiles, _, rows, _ = band_w.shape
    total = far_tile.shape[0]
    extra = total // CAP
    depth = CAP * far_w.shape[1]
    table = -(-((tiles + extra) * CAP + extra + 1) // 128) * 128
    wide = (tiles, rows, 3 * rows + depth)
    more = (extra, rows, depth)
    return pl.pallas_call(
        prep_kernel,
        out_shape=(
            pltpu.HBM((table,), jnp.int32),
            jax.ShapeDtypeStruct((rows, rows), F32),
            pltpu.HBM(wide, BF16),
            pltpu.HBM(more, BF16),
        ),
        in_specs=[SMEM, SMEM, VMEM, VMEM, ANY],
        out_specs=(ANY, VMEM, ANY, ANY),
        scratch_shapes=[
            pltpu.SMEM((table,), jnp.int32),
            pltpu.SMEM((tiles + extra,), jnp.int32),
            pltpu.SMEM((tiles + extra,), jnp.int32),
            pltpu.VMEM(band_w.shape, BF16),
            pltpu.VMEM(wide, BF16),
            pltpu.VMEM(more, BF16),
            pltpu.VMEM((tiles, rows, rows), F32),
            DMA,
            DMA((tiles // GROUP,)),
            DMA,
            DMA,
        ],
        cost_estimate=pl.CostEstimate(flops=10_000_000_000, bytes_accessed=16_000_000, transcendentals=0),
        compiler_params=pltpu.CompilerParams(vmem_limit_bytes=32 * MIB),
        name="prep",
    )(far_tile, far_count, seed_rows, far_w, in_hbm(band_w))


def change_kernel(cur_hbm, old_hbm, res_ref, cur_ref, old_ref, part_ref, sem):
    groups = sem.shape[1]
    rows = cur_ref.shape[0] // part_ref.shape[0]
    span = cur_ref.shape[0] // groups

    def copies(g):
        here = pl.ds(g * span, span)
        return (
            pltpu.make_async_copy(cur_hbm.at[here], cur_ref.at[here], sem.at[0, g]),
            pltpu.make_async_copy(old_hbm.at[here], old_ref.at[here], sem.at[1, g]),
        )

    for g in range(groups):
        for copy in copies(g):
            copy.start()

    def step(g):
        for copy in copies(g):
            copy.wait()

        def tile(t):
            place = pl.ds(pl.multiple_of(t * rows, rows), rows)
            part_ref[t] = gap_sum(cur_ref[place, :], old_ref[place, :], part_ref.shape[1:])

        loop(g * (span // rows), (g + 1) * (span // rows), tile)

    loop(0, groups, step)
    res_ref[...] = lane_totals(part_ref[...])


def change_sums(current, old, rows, groups):
    return pl.pallas_call(
        change_kernel,
        out_shape=jax.ShapeDtypeStruct((1, rows), F32),
        in_specs=[ANY, ANY],
        out_specs=VMEM,
        scratch_shapes=[
            pltpu.VMEM(current.shape, BF16),
            pltpu.VMEM(current.shape, BF16),
            pltpu.VMEM((current.shape[0] // rows, 8, rows), F32),
            DMA((2, groups)),
        ],
        cost_estimate=pl.CostEstimate(flops=5_000_000_000, bytes_accessed=8_000_000, transcendentals=0),
        compiler_params=pltpu.CompilerParams(vmem_limit_bytes=32 * MIB),
        name="change",
    )(in_hbm(current), in_hbm(old))


def spread_kernel(first, *refs):
    if first:
        (table_hbm, req_hbm, aux_ref, low_ref, high_ref, recv_ref, wide_hbm, more_hbm, cur_hbm,
         new_hbm, send_hbm, top_ref, end_ref,
         table_ref, wide_ref, more_ref, cur_ref, new_ref, far_ref, in_sem, more_sem, out_sem, table_sem,
         req_ref, side_sem, send_ref, send_sem) = refs
    else:
        (table_hbm, res_ref, aux_ref, low_ref, high_ref, recv_ref, wide_hbm, more_hbm, cur_hbm,
         new_hbm, both_hbm,
         table_ref, wide_ref, more_ref, cur_ref, new_ref, far_ref, in_sem, more_sem, out_sem, table_sem,
         both_ref, side_sem, part_ref) = refs
    tiles, rows, width = wide_ref.shape
    extra = more_ref.shape[0]
    classes = cur_ref.shape[1]
    ext_at, used_at = (tiles + extra) * CAP, (tiles + extra) * CAP + extra
    block = new_ref.shape[1]
    per = rows // block
    groups = tiles // GROUP
    span = GROUP * rows

    def get_cur(g):
        start = pl.multiple_of(g * span, span)
        return pltpu.make_async_copy(cur_hbm.at[pl.ds(start, span)], cur_ref.at[pl.ds(start + rows, span)], in_sem.at[0, g])

    def get_wide(g):
        here = pl.ds(g * GROUP, GROUP)
        return pltpu.make_async_copy(wide_hbm.at[here], wide_ref.at[here], in_sem.at[1, g])

    def fetch(g):
        get_wide(g).start()

        @pl.when(g + 1 < groups)
        def _():
            get_cur(g + 1).start()

    get_table = pltpu.make_async_copy(table_hbm, table_ref, table_sem)
    get_table.start()
    if first:
        get_req = pltpu.make_async_copy(req_hbm, req_ref, side_sem)
        get_req.start()
    get_cur(0).start()
    for g in range(AHEAD):
        fetch(g)
    cur_ref[0:rows, :] = low_ref[...]
    cur_ref[(tiles + 1) * rows :, :] = high_ref[...]
    get_table.wait()
    get_more = pltpu.make_async_copy(more_hbm, more_ref, more_sem)

    @pl.when(table_ref[used_at] > 0)
    def _():
        get_more.start()
        get_more.wait()

    lane = lax.broadcasted_iota(jnp.int32, (rows, rows), 1)

    def gathered(c):
        parts = [recv_ref[table_ref[c * CAP + p]].astype(F32) for p in range(CAP)]
        return jnp.concatenate(parts, axis=0).astype(BF16)

    def put_new(g):
        here = pl.ds(g * GROUP * per, GROUP * per)
        return pltpu.make_async_copy(new_ref.at[here], new_hbm.at[here], out_sem.at[g])

    def total(t):
        near = cur_ref[pl.ds(pl.multiple_of(t * rows, rows), 3 * rows), :]
        return dot(wide_ref[t], jnp.concatenate([near, far_ref[t]], axis=0))

    def finish(t, acc):
        cap = jnp.sum(jnp.where(lane == t, aux_ref[...], 0.0), axis=1, keepdims=True)
        mean = jnp.sum(acc * acc, axis=1, keepdims=True) * (1.0 / classes)
        scale = jnp.where(cap < 0.0, 1.0, jnp.minimum(lax.rsqrt(mean), cap))
        fresh = acc * scale
        here = pl.ds(t * per, per)
        if first:
            new_ref[here] = fresh.reshape(per, block, classes).astype(BF16)
        else:
            new_ref[here] = fresh.reshape(per, block, classes).astype(BF16)
            old = cur_ref[pl.ds(pl.multiple_of((t + 1) * rows, rows), rows), :]
            part_ref[t] = gap_sum(fresh.astype(BF16), old, part_ref.shape[1:])

    def patch(t, used):
        acc = total(t)

        def add(c, acc):
            part = dot(more_ref[c], gathered(tiles + c))
            return acc + jnp.where(table_ref[ext_at + c] == t, part, 0.0)

        finish(t, lax.fori_loop(0, used, add, acc))

    def place(t):
        far_ref[t] = gathered(t)

    loop(0, tiles, place, unroll=2)
    get_cur(0).wait()

    def ready(g):
        @pl.when(g + AHEAD < groups)
        def _():
            fetch(g + AHEAD)

        get_wide(g).wait()

        @pl.when(g + 1 < groups)
        def _():
            get_cur(g + 1).wait()

    def big_step(b):
        for i in range(UNROLL // GROUP):
            ready(b * (UNROLL // GROUP) + i)

        for i in range(UNROLL):
            finish(b * UNROLL + i, total(b * UNROLL + i))
            if i % GROUP == GROUP - 1:
                put_new(b * (UNROLL // GROUP) + i // GROUP).start()
        used = table_ref[used_at]

        def redo(c):
            t = table_ref[ext_at + c]

            def same(k, hits):
                return hits + jnp.where(table_ref[ext_at + k] == t, 1, 0)

            @pl.when((lax.div(t, UNROLL) == b) & (lax.fori_loop(0, c, same, 0) == 0))
            def _():
                put_new(lax.div(t, GROUP)).wait()
                patch(t, used)
                put_new(lax.div(t, GROUP)).start()

        loop(0, used, redo)

    loop(0, tiles // UNROLL, big_step)
    if first:
        get_req.wait()
        slots = req_ref.shape[0]
        parts = send_sem.shape[0]
        batch = send_ref.shape[1]
        share = send_ref.shape[0] // parts

        def send_copy(part):
            here = pl.ds(part * share, share)
            return pltpu.make_async_copy(send_ref.at[here], send_hbm.at[here], send_sem.at[part])

        def choose(i):
            for j in range(batch):
                send_ref[i, j] = new_ref[req_ref[j % slots, i * (batch // slots) + j // slots]]

        for part in range(parts):
            loop(part * share, (part + 1) * share, choose)
            send_copy(part).start()
        top_ref[...] = new_ref[0:per]
        end_ref[...] = new_ref[(tiles - 1) * per :]
        for part in range(parts):
            send_copy(part).wait()
    else:
        both_ref[0:1, :] = res_ref[:, :tiles]
        both_ref[1:2, :] = lane_totals(part_ref[...])[:, :tiles]
        put_both = pltpu.make_async_copy(both_ref, both_hbm, side_sem)
        put_both.start()
        put_both.wait()
    loop(0, groups, lambda g: put_new(g).wait())


def spread_call(first, table, side, aux, low, high, recv, wide, more, current):
    tiles, rows, _ = wide.shape
    total, block, classes = recv.shape
    blocks = pltpu.HBM((tiles * rows // block, block, classes), BF16)
    half = jax.ShapeDtypeStruct((rows // block, block, classes), BF16)
    picked = pltpu.HBM((total // CAP, CAP, block, classes), BF16)
    scratch = [
        pltpu.SMEM(table.shape, jnp.int32),
        pltpu.VMEM(wide.shape, BF16),
        pltpu.VMEM(more.shape, BF16),
        pltpu.VMEM(((tiles + 2) * rows, classes), BF16),
        pltpu.VMEM(blocks.shape, BF16),
        pltpu.VMEM((tiles, CAP * block, classes), BF16),
        DMA((2, tiles // GROUP)),
        DMA,
        DMA((tiles // GROUP,)),
        DMA,
    ]
    if first:
        outs, specs = (blocks, picked, half, half), (ANY, ANY, VMEM, VMEM)
        scratch += [pltpu.SMEM(side.shape, jnp.int32), DMA, pltpu.VMEM(picked.shape, BF16), DMA((8,))]
        side = in_hbm(side)
    else:
        outs, specs = (blocks, pltpu.HBM((ITERS, tiles), F32)), (ANY, ANY)
        scratch += [pltpu.VMEM((ITERS, tiles), F32), DMA, pltpu.VMEM((tiles, 8, rows), F32)]
    return pl.pallas_call(
        lambda *refs: spread_kernel(first, *refs),
        out_shape=outs,
        in_specs=[ANY, ANY if first else VMEM] + [VMEM] * 4 + [ANY] * 3,
        out_specs=specs,
        scratch_shapes=scratch,
        cost_estimate=pl.CostEstimate(flops=4_000_000_000, bytes_accessed=18_000_000, transcendentals=0),
        compiler_params=pltpu.CompilerParams(vmem_limit_bytes=32 * MIB),
        name="spread_first" if first else "spread_last",
    )(in_hbm(table), side, aux, low, high, in_vmem(recv), in_hbm(wide), in_hbm(more), in_hbm(current))


def halos(first, last):
    count = lax.axis_size("node")
    forward = [(i, (i + 1) % count) for i in range(count)]
    backward = [(target, source) for source, target in forward]
    return lax.ppermute(last, "node", forward), lax.ppermute(first, "node", backward)


def body(labels, seed_mask, band_w, far_block, far_tile, far_count, far_w):
    node_rows, classes = labels.shape
    tiles, _, rows, _ = band_w.shape
    _, peers, slots, block, _ = far_w.shape
    total = peers * slots
    got = lax.all_to_all(far_block, "node", split_axis=1, concat_axis=0, tiled=True)
    blocks = labels.reshape(-1, block, classes)
    requests, send = pick_blocks(got, blocks)

    def exchange(x):
        x = x.reshape(peers, slots, block, classes)
        return lax.all_to_all(x, "node", split_axis=0, concat_axis=0, tiled=True).reshape(total, block, classes)

    recv = exchange(send)
    low, high = halos(labels[:rows], labels[-rows:])
    table, aux, wide, more = prepare(
        far_tile[0].T.reshape(total), far_count[0], far_w.reshape(total, block, rows), band_w, seed_mask.reshape(tiles, 1, rows)
    )
    new, send, top, end = spread_call(True, table, requests, aux, low, high, recv, wide, more, labels)
    recv = exchange(send)
    low, high = halos(top.reshape(rows, classes), end.reshape(rows, classes))
    current = new.reshape(node_rows, classes)
    change = change_sums(current, labels, rows, tiles // GROUP)
    final, both = spread_call(False, table, change, aux, low, high, recv, wide, more, current)
    return final.reshape(node_rows, classes), both


def solution(mesh):
    placed = (
        P("node", None),
        P("node"),
        P("node", None, None, None),
        P("node", None, None),
        P("node", None, None),
        P("node", None),
        P("node", None, None, None, None),
    )
    return jax.shard_map(
        body,
        mesh=mesh,
        in_specs=placed,
        out_specs=(P("node", None), P(None, "node")),
        check_vma=False,
    )
```

```python
import jax
import jax.numpy as jnp
from jax import lax
from jax.experimental import pallas as pl
from jax.experimental.pallas import tpu as pltpu
from jax.sharding import PartitionSpec as P

ITERS = 2
CAP = 16
GROUP = 4
AHEAD = 7
UNROLL = 8
F32 = jnp.float32
BF16 = jnp.bfloat16
VMEM = pl.BlockSpec(memory_space=pltpu.VMEM)
SMEM = pl.BlockSpec(memory_space=pltpu.SMEM)
ANY = pl.BlockSpec(memory_space=pltpu.HBM)
MIB = 1 << 20
DMA = pltpu.SemaphoreType.DMA


def in_hbm(x):
    return pltpu.with_memory_space_constraint(x, pltpu.HBM)


def in_vmem(x):
    return pltpu.with_memory_space_constraint(x, pltpu.VMEM)


def dot(a, b):
    return jnp.dot(a, b, preferred_element_type=F32)


def loop(low, high, step, unroll=1):
    def run(i, carry):
        step(i)
        return carry

    lax.fori_loop(low, high, run, 0, unroll=unroll)


def gap_sum(new, old, shape):
    gap = jnp.abs(new - old).astype(F32)
    total = jnp.zeros(shape, F32)
    for j in range(gap.shape[1] // shape[1]):
        column = gap[:, j * shape[1] : (j + 1) * shape[1]]
        total = total + jnp.sum(column.reshape(-1, *shape), axis=0)
    return total


def lane_totals(parts):
    sums = jnp.sum(parts, axis=1)
    tiles, lanes = sums.shape
    square = jnp.concatenate([sums, jnp.zeros((lanes - tiles, lanes), F32)], axis=0)
    return jnp.sum(square.T, axis=0, keepdims=True)


def pick_kernel(got_ref, cur_ref, req_hbm, send_ref, flat_ref, req_ref, held_ref, word_sem, in_sem, out_sem):
    slots, peers = req_ref.shape
    table = jnp.concatenate([got_ref[:, 0, :], jnp.zeros((peers, peers - slots), jnp.int32)], axis=1)
    flat_ref[...] = table.T[:8, :]
    move = pltpu.make_async_copy(flat_ref.at[pl.ds(0, slots)], req_ref, word_sem)
    move.start()
    move.wait()
    keep = pltpu.make_async_copy(req_ref, req_hbm, word_sem)
    keep.start()
    parts = in_sem.shape[0]
    batch = held_ref.shape[1] // slots
    share = held_ref.shape[0] // parts

    def fetch(i, part):
        for j in range(batch):
            for k in range(slots):
                row = req_ref[k, i * batch + j]
                pltpu.make_async_copy(cur_ref.at[row], held_ref.at[i, j * slots + k], in_sem.at[part]).start()

    for part in range(parts):
        loop(part * share, (part + 1) * share, lambda i: fetch(i, part))
    for part in range(parts):
        here = pl.ds(part * share, share)
        pltpu.make_async_copy(held_ref.at[here], held_ref.at[here], in_sem.at[part]).wait()
        pltpu.make_async_copy(held_ref.at[here], send_ref.at[here], out_sem.at[part]).start()
    for part in range(parts):
        here = pl.ds(part * share, share)
        pltpu.make_async_copy(held_ref.at[here], send_ref.at[here], out_sem.at[part]).wait()
    keep.wait()


def pick_blocks(got, blocks):
    peers, _, slots = got.shape
    shape = (peers * slots // CAP, CAP) + blocks.shape[1:]
    return pl.pallas_call(
        pick_kernel,
        out_shape=(pltpu.HBM((slots, peers), jnp.int32), pltpu.HBM(shape, BF16)),
        in_specs=[VMEM, ANY],
        out_specs=(ANY, ANY),
        scratch_shapes=[
            pltpu.VMEM((8, peers), jnp.int32),
            pltpu.SMEM((slots, peers), jnp.int32),
            pltpu.VMEM(shape, BF16),
            DMA,
            DMA((4,)),
            DMA((4,)),
        ],
        cost_estimate=pl.CostEstimate(flops=1_000_000_000, bytes_accessed=4_000_000, transcendentals=0),
        compiler_params=pltpu.CompilerParams(vmem_limit_bytes=32 * MIB),
        name="pick",
    )(in_vmem(got), in_hbm(blocks))


def prep_kernel(
    tile_ref, count_ref, seed_ref, far_ref, band_hbm,
    table_hbm, aux_ref, wide_hbm, more_hbm,
    table_ref, cnt_ref, num_ref, band_ref, wide_ref, more_ref, deg_ref, in_sem, out_sem, more_sem, table_sem,
):
    peers = count_ref.shape[0]
    total = tile_ref.shape[0]
    slots = total // peers
    tiles, _, rows, _ = band_ref.shape
    chunks = tiles + more_ref.shape[0]
    ext_at, used_at = chunks * CAP, chunks * CAP + more_ref.shape[0]
    get_band = pltpu.make_async_copy(band_hbm, band_ref, in_sem)
    get_band.start()

    def clear(i):
        table_ref[i] = 0

    loop(0, table_ref.shape[0], clear, unroll=16)

    def clear_count(i):
        cnt_ref[i] = 0
        num_ref[i] = 0

    loop(0, chunks, clear_count, unroll=8)

    def scan(peer):
        live = count_ref[peer]
        for k in range(slots):
            @pl.when(k < live)
            def _():
                tile = tile_ref[k * peers + peer]
                place = num_ref[tile]
                num_ref[tile] = place + 1
                slot = peer * slots + k

                @pl.when(place < CAP)
                def _():
                    table_ref[tile * CAP + place] = slot

                @pl.when(place >= CAP)
                def _():
                    inner = lax.rem(place, CAP)

                    @pl.when(inner == 0)
                    def _():
                        fresh = table_ref[used_at]
                        table_ref[ext_at + fresh] = tile
                        table_ref[used_at] = fresh + 1

                    def find(c, last):
                        return jnp.where(table_ref[ext_at + c] == tile, c, last)

                    chunk = tiles + lax.fori_loop(0, table_ref[used_at], find, 0)
                    table_ref[chunk * CAP + inner] = slot
                    cnt_ref[chunk] = inner + 1

    loop(0, peers, scan, unroll=2)

    put_table = pltpu.make_async_copy(table_ref, table_hbm, table_sem)
    put_table.start()

    def tidy(t):
        cnt_ref[t] = jnp.minimum(num_ref[t], CAP)

    loop(0, tiles, tidy)

    def seeded(t):
        return jnp.broadcast_to(seed_ref[t].astype(F32), (rows, rows)).T == 1.0

    def weights(c):
        parts = [far_ref[table_ref[c * CAP + p]].astype(F32) for p in range(CAP)]
        mat = jnp.concatenate(parts, axis=0)
        depth = lax.broadcasted_iota(jnp.int32, mat.shape, 0)
        return jnp.where(depth < cnt_ref[c] * far_ref.shape[1], mat, 0.0).T

    get_band.wait()
    groups = tiles // GROUP

    def put_wide(g):
        here = pl.ds(g * GROUP, GROUP)
        return pltpu.make_async_copy(wide_ref.at[here], wide_hbm.at[here], out_sem.at[g])

    lane = lax.broadcasted_iota(jnp.int32, (rows, rows), 1)
    eye = (lane == lax.broadcasted_iota(jnp.int32, (rows, rows), 0)).astype(F32)

    def tile_step(t):
        seed = seeded(t)
        near = [band_ref[t, o].astype(F32) for o in range(3)]
        far = weights(t)
        degree = jnp.sum(near[0] + near[1] + near[2] + far, axis=1, keepdims=True)
        deg_ref[t] = jnp.broadcast_to(degree, (rows, rows))
        for j, (kept, other) in enumerate(zip(near + [far], (0.0, eye, 0.0, 0.0))):
            wide_ref[t, :, j * rows : (j + 1) * rows] = jnp.where(seed, other, kept).astype(BF16)

    def group_step(g):
        for i in range(GROUP):
            tile_step(g * GROUP + i)
        put_wide(g).start()

    loop(0, groups, group_step)

    def extra_step(c):
        t = table_ref[ext_at + c]
        mat = weights(tiles + c)
        more_ref[c] = jnp.where(seeded(t), 0.0, mat).astype(BF16)
        deg_ref[t] = deg_ref[t] + jnp.sum(mat, axis=1, keepdims=True)

    loop(0, table_ref[used_at], extra_step)
    put_more = pltpu.make_async_copy(more_ref, more_hbm, more_sem)
    put_more.start()
    aux_ref[...] = jnp.ones_like(aux_ref)

    def finish(t):
        cap = 1.0 / deg_ref[t] / 0.05
        aux_ref[...] = jnp.where(lane == t, jnp.where(seeded(t), -1.0, cap), aux_ref[...])

    loop(0, tiles, finish, unroll=2)
    loop(0, groups, lambda g: put_wide(g).wait())
    put_more.wait()
    put_table.wait()


def prepare(far_tile, far_count, far_w, band_w, seed_rows):
    tiles, _, rows, _ = band_w.shape
    total = far_tile.shape[0]
    extra = total // CAP
    depth = CAP * far_w.shape[1]
    table = -(-((tiles + extra) * CAP + extra + 1) // 128) * 128
    wide = (tiles, rows, 3 * rows + depth)
    more = (extra, rows, depth)
    return pl.pallas_call(
        prep_kernel,
        out_shape=(
            pltpu.HBM((table,), jnp.int32),
            jax.ShapeDtypeStruct((rows, rows), F32),
            pltpu.HBM(wide, BF16),
            pltpu.HBM(more, BF16),
        ),
        in_specs=[SMEM, SMEM, VMEM, VMEM, ANY],
        out_specs=(ANY, VMEM, ANY, ANY),
        scratch_shapes=[
            pltpu.SMEM((table,), jnp.int32),
            pltpu.SMEM((tiles + extra,), jnp.int32),
            pltpu.SMEM((tiles + extra,), jnp.int32),
            pltpu.VMEM(band_w.shape, BF16),
            pltpu.VMEM(wide, BF16),
            pltpu.VMEM(more, BF16),
            pltpu.VMEM((tiles, rows, rows), F32),
            DMA,
            DMA((tiles // GROUP,)),
            DMA,
            DMA,
        ],
        cost_estimate=pl.CostEstimate(flops=10_000_000_000, bytes_accessed=16_000_000, transcendentals=0),
        compiler_params=pltpu.CompilerParams(vmem_limit_bytes=32 * MIB),
        name="prep",
    )(far_tile, far_count, seed_rows, far_w, in_hbm(band_w))


def change_kernel(cur_hbm, old_hbm, res_ref, cur_ref, old_ref, part_ref, sem):
    groups = sem.shape[1]
    rows = cur_ref.shape[0] // part_ref.shape[0]
    span = cur_ref.shape[0] // groups

    def copies(g):
        here = pl.ds(g * span, span)
        return (
            pltpu.make_async_copy(cur_hbm.at[here], cur_ref.at[here], sem.at[0, g]),
            pltpu.make_async_copy(old_hbm.at[here], old_ref.at[here], sem.at[1, g]),
        )

    for g in range(groups):
        for copy in copies(g):
            copy.start()

    def step(g):
        for copy in copies(g):
            copy.wait()

        def tile(t):
            place = pl.ds(pl.multiple_of(t * rows, rows), rows)
            part_ref[t] = gap_sum(cur_ref[place, :], old_ref[place, :], part_ref.shape[1:])

        loop(g * (span // rows), (g + 1) * (span // rows), tile)

    loop(0, groups, step)
    res_ref[...] = lane_totals(part_ref[...])


def change_sums(current, old, rows, groups):
    return pl.pallas_call(
        change_kernel,
        out_shape=jax.ShapeDtypeStruct((1, rows), F32),
        in_specs=[ANY, ANY],
        out_specs=VMEM,
        scratch_shapes=[
            pltpu.VMEM(current.shape, BF16),
            pltpu.VMEM(current.shape, BF16),
            pltpu.VMEM((current.shape[0] // rows, 8, rows), F32),
            DMA((2, groups)),
        ],
        cost_estimate=pl.CostEstimate(flops=5_000_000_000, bytes_accessed=8_000_000, transcendentals=0),
        compiler_params=pltpu.CompilerParams(vmem_limit_bytes=32 * MIB),
        name="change",
    )(in_hbm(current), in_hbm(old))


def spread_kernel(first, *refs):
    if first:
        (table_hbm, req_hbm, aux_ref, low_ref, high_ref, recv_ref, wide_hbm, more_hbm, cur_hbm,
         new_hbm, send_hbm, top_ref, end_ref,
         table_ref, wide_ref, more_ref, cur_ref, new_ref, far_ref, in_sem, more_sem, out_sem, table_sem,
         req_ref, side_sem, send_ref, send_sem) = refs
    else:
        (table_hbm, res_ref, aux_ref, low_ref, high_ref, recv_ref, wide_hbm, more_hbm, cur_hbm,
         new_hbm, both_hbm,
         table_ref, wide_ref, more_ref, cur_ref, new_ref, far_ref, in_sem, more_sem, out_sem, table_sem,
         both_ref, side_sem, part_ref) = refs
    tiles, rows, width = wide_ref.shape
    extra = more_ref.shape[0]
    classes = cur_ref.shape[1]
    ext_at, used_at = (tiles + extra) * CAP, (tiles + extra) * CAP + extra
    block = new_ref.shape[1]
    per = rows // block
    groups = tiles // GROUP
    span = GROUP * rows

    def get_cur(g):
        start = pl.multiple_of(g * span, span)
        return pltpu.make_async_copy(cur_hbm.at[pl.ds(start, span)], cur_ref.at[pl.ds(start + rows, span)], in_sem.at[0, g])

    def get_wide(g):
        here = pl.ds(g * GROUP, GROUP)
        return pltpu.make_async_copy(wide_hbm.at[here], wide_ref.at[here], in_sem.at[1, g])

    def fetch(g):
        get_wide(g).start()

        @pl.when(g + 1 < groups)
        def _():
            get_cur(g + 1).start()

    get_table = pltpu.make_async_copy(table_hbm, table_ref, table_sem)
    get_table.start()
    if first:
        get_req = pltpu.make_async_copy(req_hbm, req_ref, side_sem)
        get_req.start()
    get_cur(0).start()
    for g in range(AHEAD):
        fetch(g)
    cur_ref[0:rows, :] = low_ref[...]
    cur_ref[(tiles + 1) * rows :, :] = high_ref[...]
    get_table.wait()
    get_more = pltpu.make_async_copy(more_hbm, more_ref, more_sem)

    @pl.when(table_ref[used_at] > 0)
    def _():
        get_more.start()
        get_more.wait()

    lane = lax.broadcasted_iota(jnp.int32, (rows, rows), 1)

    def gathered(c):
        parts = [recv_ref[table_ref[c * CAP + p]].astype(F32) for p in range(CAP)]
        return jnp.concatenate(parts, axis=0).astype(BF16)

    def put_new(g):
        here = pl.ds(g * GROUP * per, GROUP * per)
        return pltpu.make_async_copy(new_ref.at[here], new_hbm.at[here], out_sem.at[g])

    def total(t):
        near = cur_ref[pl.ds(pl.multiple_of(t * rows, rows), 3 * rows), :]
        return dot(wide_ref[t], jnp.concatenate([near, far_ref[t]], axis=0))

    def finish(t, acc):
        cap = jnp.sum(jnp.where(lane == t, aux_ref[...], 0.0), axis=1, keepdims=True)
        mean = jnp.sum(acc * acc, axis=1, keepdims=True) * (1.0 / classes)
        scale = jnp.where(cap < 0.0, 1.0, jnp.minimum(lax.rsqrt(mean), cap))
        fresh = acc * scale
        here = pl.ds(t * per, per)
        if first:
            new_ref[here] = fresh.reshape(per, block, classes).astype(BF16)
        else:
            new_ref[here] = fresh.reshape(per, block, classes).astype(BF16)
            old = cur_ref[pl.ds(pl.multiple_of((t + 1) * rows, rows), rows), :]
            part_ref[t] = gap_sum(fresh.astype(BF16), old, part_ref.shape[1:])

    def patch(t, used):
        acc = total(t)

        def add(c, acc):
            part = dot(more_ref[c], gathered(tiles + c))
            return acc + jnp.where(table_ref[ext_at + c] == t, part, 0.0)

        finish(t, lax.fori_loop(0, used, add, acc))

    def place(t):
        far_ref[t] = gathered(t)

    loop(0, tiles, place, unroll=4)
    get_cur(0).wait()

    def ready(g):
        @pl.when(g + AHEAD < groups)
        def _():
            fetch(g + AHEAD)

        get_wide(g).wait()

        @pl.when(g + 1 < groups)
        def _():
            get_cur(g + 1).wait()

    def big_step(b):
        for i in range(UNROLL // GROUP):
            ready(b * (UNROLL // GROUP) + i)

        for i in range(UNROLL):
            finish(b * UNROLL + i, total(b * UNROLL + i))
            if i % GROUP == GROUP - 1:
                put_new(b * (UNROLL // GROUP) + i // GROUP).start()
        used = table_ref[used_at]

        def redo(c):
            t = table_ref[ext_at + c]

            def same(k, hits):
                return hits + jnp.where(table_ref[ext_at + k] == t, 1, 0)

            @pl.when((lax.div(t, UNROLL) == b) & (lax.fori_loop(0, c, same, 0) == 0))
            def _():
                put_new(lax.div(t, GROUP)).wait()
                patch(t, used)
                put_new(lax.div(t, GROUP)).start()

        loop(0, used, redo)

    loop(0, tiles // UNROLL, big_step)
    if first:
        get_req.wait()
        slots = req_ref.shape[0]
        parts = send_sem.shape[0]
        batch = send_ref.shape[1]
        share = send_ref.shape[0] // parts

        def send_copy(part):
            here = pl.ds(part * share, share)
            return pltpu.make_async_copy(send_ref.at[here], send_hbm.at[here], send_sem.at[part])

        def choose(i):
            for j in range(batch):
                send_ref[i, j] = new_ref[req_ref[j % slots, i * (batch // slots) + j // slots]]

        for part in range(parts):
            loop(part * share, (part + 1) * share, choose)
            send_copy(part).start()
        top_ref[...] = new_ref[0:per]
        end_ref[...] = new_ref[(tiles - 1) * per :]
        for part in range(parts):
            send_copy(part).wait()
    else:
        both_ref[0:1, :] = res_ref[:, :tiles]
        both_ref[1:2, :] = lane_totals(part_ref[...])[:, :tiles]
        put_both = pltpu.make_async_copy(both_ref, both_hbm, side_sem)
        put_both.start()
        put_both.wait()
    loop(0, groups, lambda g: put_new(g).wait())


def spread_call(first, table, side, aux, low, high, recv, wide, more, current):
    tiles, rows, _ = wide.shape
    total, block, classes = recv.shape
    blocks = pltpu.HBM((tiles * rows // block, block, classes), BF16)
    half = jax.ShapeDtypeStruct((rows // block, block, classes), BF16)
    picked = pltpu.HBM((total // CAP, CAP, block, classes), BF16)
    scratch = [
        pltpu.SMEM(table.shape, jnp.int32),
        pltpu.VMEM(wide.shape, BF16),
        pltpu.VMEM(more.shape, BF16),
        pltpu.VMEM(((tiles + 2) * rows, classes), BF16),
        pltpu.VMEM(blocks.shape, BF16),
        pltpu.VMEM((tiles, CAP * block, classes), BF16),
        DMA((2, tiles // GROUP)),
        DMA,
        DMA((tiles // GROUP,)),
        DMA,
    ]
    if first:
        outs, specs = (blocks, picked, half, half), (ANY, ANY, VMEM, VMEM)
        scratch += [pltpu.SMEM(side.shape, jnp.int32), DMA, pltpu.VMEM(picked.shape, BF16), DMA((8,))]
        side = in_hbm(side)
    else:
        outs, specs = (blocks, pltpu.HBM((ITERS, tiles), F32)), (ANY, ANY)
        scratch += [pltpu.VMEM((ITERS, tiles), F32), DMA, pltpu.VMEM((tiles, 8, rows), F32)]
    return pl.pallas_call(
        lambda *refs: spread_kernel(first, *refs),
        out_shape=outs,
        in_specs=[ANY, ANY if first else VMEM] + [VMEM] * 4 + [ANY] * 3,
        out_specs=specs,
        scratch_shapes=scratch,
        cost_estimate=pl.CostEstimate(flops=4_000_000_000, bytes_accessed=18_000_000, transcendentals=0),
        compiler_params=pltpu.CompilerParams(vmem_limit_bytes=32 * MIB),
        name="spread_first" if first else "spread_last",
    )(in_hbm(table), side, aux, low, high, in_vmem(recv), in_hbm(wide), in_hbm(more), in_hbm(current))


def halos(first, last):
    count = lax.axis_size("node")
    forward = [(i, (i + 1) % count) for i in range(count)]
    backward = [(target, source) for source, target in forward]
    return lax.ppermute(last, "node", forward), lax.ppermute(first, "node", backward)


def body(labels, seed_mask, band_w, far_block, far_tile, far_count, far_w):
    node_rows, classes = labels.shape
    tiles, _, rows, _ = band_w.shape
    _, peers, slots, block, _ = far_w.shape
    total = peers * slots
    got = lax.all_to_all(far_block, "node", split_axis=1, concat_axis=0, tiled=True)
    blocks = labels.reshape(-1, block, classes)
    requests, send = pick_blocks(got, blocks)

    def exchange(x):
        x = x.reshape(peers, slots, block, classes)
        return lax.all_to_all(x, "node", split_axis=0, concat_axis=0, tiled=True).reshape(total, block, classes)

    recv = exchange(send)
    low, high = halos(labels[:rows], labels[-rows:])
    table, aux, wide, more = prepare(
        far_tile[0].T.reshape(total), far_count[0], far_w.reshape(total, block, rows), band_w, seed_mask.reshape(tiles, 1, rows)
    )
    new, send, top, end = spread_call(True, table, requests, aux, low, high, recv, wide, more, labels)
    recv = exchange(send)
    low, high = halos(top.reshape(rows, classes), end.reshape(rows, classes))
    current = new.reshape(node_rows, classes)
    change = change_sums(current, labels, rows, tiles // GROUP)
    final, both = spread_call(False, table, change, aux, low, high, recv, wide, more, current)
    return final.reshape(node_rows, classes), both


def solution(mesh):
    placed = (
        P("node", None),
        P("node"),
        P("node", None, None, None),
        P("node", None, None),
        P("node", None, None),
        P("node", None),
        P("node", None, None, None, None),
    )
    return jax.shard_map(
        body,
        mesh=mesh,
        in_specs=placed,
        out_specs=(P("node", None), P(None, "node")),
        check_vma=False,
    )
```
